32 devices in a mesh: rep: 4 (over x, y), dp: 8 (over z, core).
Axes of the slice: x: 2, y: 2, z: 4, core: 2. Of those that a mesh axis runs over, the one named last changes fastest.
Arguments:
- g_w_gate: bfloat16 [32, 2, 1024, 3584], P(('rep', 'dp')), parts along dimension 0
- g_w_up: bfloat16 [32, 2, 1024, 3584], P(('rep', 'dp')), parts along dimension 0
- g_w_down: bfloat16 [32, 2, 3584, 1024], P(('rep', 'dp')), parts along dimension 0
- w_gate: bfloat16 [2, 1024, 3584], replicated
- w_up: bfloat16 [2, 1024, 3584], replicated
- w_down: bfloat16 [2, 3584, 1024], replicated
- m_w_gate: float32 [2, 1024, 3584], P(None, 'dp')
- m_w_up: float32 [2, 1024, 3584], P(None, 'dp')
- m_w_down: float32 [2, 3584, 1024], P(None, 'dp')
- v_w_gate: float32 [2, 1024, 3584], P(None, 'dp')
- v_w_up: float32 [2, 1024, 3584], P(None, 'dp')
- v_w_down: float32 [2, 3584, 1024], P(None, 'dp')
Outputs:
- output 1: bfloat16 [8, 1024, 3584], P('rep'), parts along dimension 0
- output 2: bfloat16 [8, 1024, 3584], P('rep'), parts along dimension 0
- output 3: bfloat16 [8, 3584, 1024], P('rep'), parts along dimension 0
- output 4: float32 [8, 1024, 3584], P('rep', 'dp'), parts along dimension 0
- output 5: float32 [8, 1024, 3584], P('rep', 'dp'), parts along dimension 0
- output 6: float32 [8, 3584, 1024], P('rep', 'dp'), parts along dimension 0
- output 7: float32 [8, 1024, 3584], P('rep', 'dp'), parts along dimension 0
- output 8: float32 [8, 1024, 3584], P('rep', 'dp'), parts along dimension 0
- output 9: float32 [8, 3584, 1024], P('rep', 'dp'), parts along dimension 0
There are 4 independent parts. The reference program is written for one: setup_inputs(seed, part) draws one part's arguments, and reference() takes and returns one part's arrays. A program takes and returns all parts, laid end to end along the dimension named above; an argument that names none is the same for every part.
All inputs are finite; a program needn't handle non-finite values.
Results may differ from the reference program's by a relative error of at most 0.022.
Values are sent between devices in bfloat16 or wider.
A program may use at most 2 GiB of HBM per device.

```python
import jax
import jax.numpy as jnp
from jax import lax

DEVICES = 8
D = 1024
FF = 3584
LAYERS = 2
NAMES = ("w_gate", "w_up", "w_down")
SHAPES = {"w_gate": (LAYERS, D, FF), "w_up": (LAYERS, D, FF), "w_down": (LAYERS, FF, D)}


def setup_inputs(seed: int = 0, part: int = 0) -> dict:
    kz, *keys = jax.random.split(jax.random.key(seed), 1 + 5 * len(NAMES))
    loud = 2.0 ** jax.random.uniform(kz, (), jnp.float32, -1.0, 1.0)
    drawn = {}
    for name, key, both in zip(NAMES, keys[:3], keys[3:6], strict=True):
        own = jax.random.normal(jax.random.fold_in(key, part), (DEVICES, *SHAPES[name]), jnp.float32)
        shared = jax.random.normal(jax.random.fold_in(both, part), SHAPES[name], jnp.float32)
        drawn["g_" + name] = (loud * (0.7 * shared / DEVICES + 0.7 * own * DEVICES**-0.5)).astype(jnp.bfloat16)
    for name, key in zip(NAMES, keys[6:9], strict=True):
        drawn[name] = (jax.random.normal(key, SHAPES[name], jnp.float32) * SHAPES[name][1] ** -0.5).astype(jnp.bfloat16)
    for name, key in zip(NAMES, keys[9:12], strict=True):
        drawn["m_" + name] = loud * 0.5 * jax.random.normal(key, SHAPES[name], jnp.float32)
    for name, key in zip(NAMES, keys[12:15], strict=True):
        drawn["v_" + name] = loud * loud * jax.random.uniform(key, SHAPES[name], jnp.float32, 0.5, 1.5)
    return drawn


def adamw(w, m, v, g):
    m = 0.9 * m + 0.1 * g
    v = 0.95 * v + 0.05 * g * g
    step = m * lax.rsqrt(v + 1e-8) + 0.1 * w
    return (w - 0.02 * step).astype(jnp.bfloat16), m, v


def reference(g_w_gate, g_w_up, g_w_down, w_gate, w_up, w_down, m_w_gate, m_w_up, m_w_down, v_w_gate, v_w_up, v_w_down):
    def total(terms):
        return lax.scan(lambda so_far, term: (so_far + term.astype(jnp.float32), None), jnp.zeros(terms.shape[1:], jnp.float32), terms)[0]

    gradients = [total(terms).astype(jnp.bfloat16).astype(jnp.float32) for terms in (g_w_gate, g_w_up, g_w_down)]
    new = [
        adamw(w.astype(jnp.float32), m, v, g)
        for w, m, v, g in zip((w_gate, w_up, w_down), (m_w_gate, m_w_up, m_w_down), (v_w_gate, v_w_up, v_w_down), gradients, strict=True)
    ]
    return tuple(one[which] for which in range(3) for one in new)
```

```python
import functools

import jax
import jax.numpy as jnp
from jax import lax
from jax.experimental import pallas as pl
from jax.experimental.pallas import tpu as pltpu
from jax.sharding import PartitionSpec as P

MESH = pl.DeviceIdType.MESH
N = 28
UNITS = 224
PER = UNITS // N
K = 6 * PER
H = 1
AHEAD = 2
EARLY = 2
LATE = 3
R = 8
CH = 7
SHAPES = ((1024, 3584), (1024, 3584), (3584, 1024))
F_OF = (3 * H, 2 * H, 2 * H, 3 * H)
STEPS = K + 6 * H + LATE + 1


def tiled(a, blocks):
    layers, rows, columns = a.shape
    a = a.reshape(layers, blocks, rows // blocks // 8, 8, columns // 128, 128).transpose(0, 1, 2, 4, 3, 5)
    return a.reshape(layers, blocks, -1, 16, 128)


def untiled(a, rows, columns):
    layers, blocks = a.shape[:2]
    a = a.reshape(layers, blocks, rows // blocks // 8, columns // 128, 8, 128).transpose(0, 1, 2, 4, 3, 5)
    return a.reshape(layers, rows, columns)


def kernel(*refs):
    g, w, m, v = refs[0:3], refs[3:6], refs[6:9], refs[9:12]
    W, MV = refs[12:14]
    own, part, inb, mvb = refs[14:18]
    own_sem, part_send, part_recv, rs_send, rs_recv, mv_load, mv_store, ag_send, ag_recv, p_send, p_recv = refs[18:]

    me = lax.axis_index("dp")
    z, c = me // 2, me % 2
    partner = me + 1 - 2 * c
    up, down = jnp.minimum(me + 2, 7), jnp.maximum(me - 2, 0)
    f_me = jnp.maximum(z, 3 - z) * H

    barrier = pltpu.get_barrier_semaphore()
    pl.semaphore_signal(barrier, inc=1, device_id={"dp": partner}, device_id_type=MESH)

    @pl.when(z < 3)
    def _():
        pl.semaphore_signal(barrier, inc=1, device_id={"dp": up}, device_id_type=MESH)

    @pl.when(z > 0)
    def _():
        pl.semaphore_signal(barrier, inc=1, device_id={"dp": down}, device_id_type=MESH)

    pl.semaphore_wait(barrier, jnp.where((z == 0) | (z == 3), 2, 3))

    def live(k):
        return (k >= 0) & (k < K)

    def place(k):
        return k // (2 * PER), (k // PER) % 2, pl.ds((k % PER) * N, N)

    def of_weight(k, do):
        for i in range(3):
            pl.when(k // (2 * PER) == i)(functools.partial(do, i))

    def remote(src, dst, send, recv, to):
        return pltpu.make_async_remote_copy(src_ref=src, dst_ref=dst, send_sem=send, recv_sem=recv, device_id={"dp": to}, device_id_type=MESH)

    def wait_unit(sem):
        pltpu.make_async_copy(inb.at[0, 0], inb.at[0, 0], sem).wait()

    def wait_own(sem):
        pltpu.make_async_copy(own.at[0], own.at[0], sem).wait()

    def wait_moment(sem):
        pltpu.make_async_copy(mvb.at[0, 0], mvb.at[0, 0], sem).wait()

    def add(slot, zp, more):
        def chunk(i, _):
            at = pl.ds(i * CH, CH)
            s = own[slot, zp, at].astype(jnp.float32) + part[slot, zp, at].astype(jnp.float32)
            for idx in more:
                s = s + inb[slot, idx, at].astype(jnp.float32)
            own[slot, zp, at] = s.astype(jnp.bfloat16)
            return 0

        lax.fori_loop(0, N // CH, chunk, 0)

    def step_on(slot, k, more):
        wt, layer, _ = place(k)
        base = (k % PER) * N

        def chunk(i, _):
            at = pl.ds(i * CH, CH)
            s = own[slot, z, at].astype(jnp.float32) + part[slot, z, at].astype(jnp.float32)
            for idx in more:
                s = s + inb[slot, idx, at].astype(jnp.float32)
            grad = s.astype(jnp.bfloat16).astype(jnp.float32)
            here = pl.ds(base + i * CH, CH)
            weight = W[wt, layer, me, here].astype(jnp.float32)
            mom = 0.9 * mvb[slot, 0, at] + 0.1 * grad
            var = 0.95 * mvb[slot, 1, at] + 0.05 * grad * grad
            mvb[slot, 0, at] = mom
            mvb[slot, 1, at] = var
            W[wt, layer, me, here] = (weight - 0.02 * (mom * lax.rsqrt(var + 1e-8) + 0.1 * weight)).astype(jnp.bfloat16)
            return 0

        lax.fori_loop(0, N // CH, chunk, 0)

    def block(k, zp, cc):
        wt, layer, at = place(k)
        return W.at[wt, layer, 2 * zp + cc, at]

    def body(t, _):
        t = t - AHEAD

        for zp in range(4):
            k = t - LATE - jnp.where(zp > z, z, 3 - z) * H

            @pl.when(live(k) & (zp != z))
            def _(k=k, zp=zp):
                wait_unit(rs_send.at[k % R, zp])

        @pl.when(live(t))
        def _():
            wait_own(own_sem.at[t % R])
            wait_own(part_recv.at[t % R])
            wait_own(part_send.at[t % R])

        ka = t + AHEAD

        @pl.when(live(ka))
        def _():
            slot = ka % R
            _, layer, at = place(ka)

            def do(i):
                pltpu.make_async_copy(g[i].at[layer, :, c, at], own.at[slot], own_sem.at[slot]).start()
                remote(g[i].at[layer, :, 1 - c, at], part.at[slot], part_send.at[slot], part_recv.at[slot], partner).start()

            of_weight(ka, do)

        ks = t - f_me - LATE

        @pl.when(live(ks))
        def _():
            wait_moment(mv_store.at[ks % R, 0])
            wait_moment(mv_store.at[ks % R, 1])

        km = t - f_me + EARLY

        @pl.when(live(km))
        def _():
            slot = km % R
            _, layer, at = place(km)

            def do(i):
                pltpu.make_async_copy(m[i].at[layer, 0, at], mvb.at[slot, 0], mv_load.at[slot, 0]).start()
                pltpu.make_async_copy(v[i].at[layer, 0, at], mvb.at[slot, 1], mv_load.at[slot, 1]).start()
                pltpu.make_async_copy(w[i].at[layer, me, at], W.at[i, layer, me, at], mv_load.at[slot, 2]).start()

            of_weight(km, do)

        ku, kd = t - z * H, t - (3 - z) * H
        for far in range(3):
            zp = 3 - far

            @pl.when(live(ku) & (zp > z))
            def _(zp=zp):
                slot = ku % R

                @pl.when(z == 0)
                def _():
                    add(slot, zp, ())

                @pl.when(z > 0)
                def _():
                    wait_unit(rs_recv.at[slot, zp])
                    add(slot, zp, (zp,))

                remote(own.at[slot, zp], inb.at[slot, zp], rs_send.at[slot, zp], rs_recv.at[slot, zp], up).start()

            zq = far

            @pl.when(live(kd) & (zq < z))
            def _(zq=zq):
                slot = kd % R

                @pl.when(z == 3)
                def _():
                    add(slot, zq, ())

                @pl.when(z < 3)
                def _():
                    wait_unit(rs_recv.at[slot, zq])
                    add(slot, zq, (zq,))

                idx = jnp.where(zq == z - 1, 4, zq)
                remote(own.at[slot, zq], inb.at[slot, idx], rs_send.at[slot, zq], rs_recv.at[slot, idx], down).start()

        kf = t - f_me

        @pl.when(live(kf))
        def _():
            slot = kf % R
            wait_moment(mv_load.at[slot, 0])
            wait_moment(mv_load.at[slot, 1])
            wait_unit(mv_load.at[slot, 2])

            @pl.when(z > 0)
            def _():
                wait_unit(rs_recv.at[slot, z])

            @pl.when(z < 3)
            def _():
                wait_unit(rs_recv.at[slot, 4])

            @pl.when(z == 0)
            def _():
                step_on(slot, kf, (4,))

            @pl.when(z == 3)
            def _():
                step_on(slot, kf, (3,))

            @pl.when((z > 0) & (z < 3))
            def _():
                step_on(slot, kf, (z, 4))

            mine = block(kf, z, c)

            @pl.when(z < 3)
            def _():
                remote(mine, mine, ag_send.at[slot, z], ag_recv.at[slot, z], up).start()

            @pl.when(z > 0)
            def _():
                remote(mine, mine, ag_send.at[slot, 4], ag_recv.at[slot, z], down).start()

            remote(mine, mine, p_send.at[slot, z], p_recv.at[slot, z], partner).start()
            wt, layer, at = place(kf)
            pltpu.make_async_copy(mvb.at[slot, 0], MV.at[0, wt, layer, at], mv_store.at[slot, 0]).start()
            pltpu.make_async_copy(mvb.at[slot, 1], MV.at[1, wt, layer, at], mv_store.at[slot, 1]).start()

        for near in range(3):
            zp = 2 - near
            kb = t - F_OF[zp] - (z - zp) * H

            @pl.when(live(kb) & (zp < z))
            def _(zp=zp, k=kb):
                slot = k % R
                wait_unit(ag_recv.at[slot, zp])
                there = block(k, zp, c)

                @pl.when(z < 3)
                def _():
                    remote(there, there, ag_send.at[slot, zp], ag_recv.at[slot, zp], up).start()

                remote(there, there, p_send.at[slot, zp], p_recv.at[slot, zp], partner).start()

            zq = 1 + near
            kc = t - F_OF[zq] - (zq - z) * H

            @pl.when(live(kc) & (zq > z))
            def _(zq=zq, k=kc):
                slot = k % R
                wait_unit(ag_recv.at[slot, zq])
                there = block(k, zq, c)

                @pl.when(z > 0)
                def _():
                    remote(there, there, ag_send.at[slot, zq], ag_recv.at[slot, zq], down).start()

                remote(there, there, p_send.at[slot, zq], p_recv.at[slot, zq], partner).start()

        for zp in range(4):
            ksent = t - F_OF[zp] - jnp.abs(z - zp) * H

            @pl.when(live(ksent - 1))
            def _(zp=zp, k=ksent - 1):
                wait_unit(p_recv.at[k % R, zp])

            @pl.when(live(ksent - LATE))
            def _(zp=zp, k=ksent - LATE):
                wait_unit(p_send.at[k % R, zp])

                @pl.when((zp < z) & (z < 3))
                def _():
                    wait_unit(ag_send.at[k % R, zp])

                @pl.when((zp > z) & (z > 0))
                def _():
                    wait_unit(ag_send.at[k % R, zp])

                @pl.when((zp == z) & (z < 3))
                def _():
                    wait_unit(ag_send.at[k % R, zp])

                @pl.when((zp == z) & (z > 0))
                def _():
                    wait_unit(ag_send.at[k % R, 4])

        return 0

    lax.fori_loop(0, STEPS + AHEAD, body, 0)


def solution(mesh):
    def step(*arrays):
        g = [tiled(a[0], 8).reshape(2, 4, 2, UNITS, 16, 128) for a in arrays[:3]]
        w = [tiled(a, 8) for a in arrays[3:6]]
        moments = [tiled(a, 1) for a in arrays[6:]]
        hbm = pl.BlockSpec(memory_space=pl.ANY)
        piece = (N, 16, 128)
        dma = pltpu.SemaphoreType.DMA
        new, mv = pl.pallas_call(
            kernel,
            out_shape=[
                jax.ShapeDtypeStruct((3, 2, 8, UNITS, 16, 128), jnp.bfloat16),
                jax.ShapeDtypeStruct((2, 3, 2, UNITS, 16, 128), jnp.float32),
            ],
            in_specs=[hbm] * 12,
            out_specs=[hbm, hbm] if False else [pl.BlockSpec(memory_space=pltpu.VMEM), hbm],
            scratch_shapes=[
                pltpu.VMEM((R, 4, *piece), jnp.bfloat16),
                pltpu.VMEM((R, 4, *piece), jnp.bfloat16),
                pltpu.VMEM((R, 5, *piece), jnp.bfloat16),
                pltpu.VMEM((R, 2, *piece), jnp.float32),
                dma((R,)),
                dma((R,)),
                dma((R,)),
                dma((R, 4)),
                dma((R, 5)),
                dma((R, 3)),
                dma((R, 2)),
                dma((R, 5)),
                dma((R, 4)),
                dma((R, 4)),
                dma((R, 4)),
            ],
            compiler_params=pltpu.CompilerParams(collective_id=0, has_side_effects=True, vmem_limit_bytes=62 * 1024 * 1024),
            name="sum_step_spread",
        )(*g, *w, *moments)
        whole = [untiled(new[i], *SHAPES[i]) for i in range(3)]
        rest = [untiled(mv[which, i][:, None], SHAPES[i][0] // 8, SHAPES[i][1]) for which in range(2) for i in range(3)]
        return (*whole, *rest)

    all_of, cut = P(None, None, None), P(None, "dp", None)
    return jax.shard_map(
        step,
        mesh=mesh,
        in_specs=(P(("rep", "dp"), None, None, None),) * 3 + (all_of,) * 3 + (cut,) * 6,
        out_specs=(P("rep", None, None),) * 3 + (P("rep", "dp", None),) * 6,
        check_vma=False,
    )
```

```python
import functools

import jax
import jax.numpy as jnp
from jax import lax
from jax.experimental import pallas as pl
from jax.experimental.pallas import tpu as pltpu
from jax.sharding import PartitionSpec as P

MESH = pl.DeviceIdType.MESH
N = 14
UNITS = 224
PER = UNITS // N
K = 6 * PER
H = 1
AHEAD = 2
EARLY = 2
LATE = 3
R = 8
CH = 7
NV = 2
LIMIT = 7.75
SHAPES = ((1024, 3584), (1024, 3584), (3584, 1024))
F_OF = (3 * H, 2 * H, 2 * H, 3 * H)
STEPS = K + 6 * H + LATE + 1


def tiled(a, blocks):
    layers, rows, columns = a.shape
    a = a.reshape(layers, blocks, rows // blocks // 8, 8, columns // 128, 128).transpose(0, 1, 2, 4, 3, 5)
    return a.reshape(layers, blocks, -1, 16, 128)


def untiled(a, rows, columns):
    layers, blocks = a.shape[:2]
    a = a.reshape(layers, blocks, rows // blocks // 8, columns // 128, 8, 128).transpose(0, 1, 2, 4, 3, 5)
    return a.reshape(layers, rows, columns)


def kernel(*refs):
    g, w, m, v = refs[0:3], refs[3:6], refs[6:9], refs[9:12]
    W, MVV, MV = refs[12:15]
    own, part, inb, mvb = refs[15:19]
    own_sem, part_send, part_recv, rs_send, rs_recv, mv_load, mv_store, ag_send, ag_recv, p_send, p_recv = refs[19:]

    me = lax.axis_index("dp")
    z, c = me // 2, me % 2
    partner = me + 1 - 2 * c
    up, down = jnp.minimum(me + 2, 7), jnp.maximum(me - 2, 0)
    f_me = jnp.maximum(z, 3 - z) * H

    barrier = pltpu.get_barrier_semaphore()
    pl.semaphore_signal(barrier, inc=1, device_id={"dp": partner}, device_id_type=MESH)

    @pl.when(z < 3)
    def _():
        pl.semaphore_signal(barrier, inc=1, device_id={"dp": up}, device_id_type=MESH)

    @pl.when(z > 0)
    def _():
        pl.semaphore_signal(barrier, inc=1, device_id={"dp": down}, device_id_type=MESH)

    pl.semaphore_wait(barrier, jnp.where((z == 0) | (z == 3), 2, 3))

    def live(k):
        return (k >= 0) & (k < K)

    def place(k):
        return k // (2 * PER), (k // PER) % 2, pl.ds((k % PER) * N, N)

    def of_weight(k, do):
        for i in range(3):
            pl.when(k // (2 * PER) == i)(functools.partial(do, i))

    def remote(src, dst, send, recv, to):
        return pltpu.make_async_remote_copy(src_ref=src, dst_ref=dst, send_sem=send, recv_sem=recv, device_id={"dp": to}, device_id_type=MESH)

    def wait_unit(sem):
        pltpu.make_async_copy(inb.at[0, 0], inb.at[0, 0], sem).wait()

    def wait_own(sem):
        pltpu.make_async_copy(own.at[0], own.at[0], sem).wait()

    def wait_moment(sem):
        pltpu.make_async_copy(mvb.at[0, 0], mvb.at[0, 0], sem).wait()

    def add(slot, zp, more):
        def chunk(i, _):
            at = pl.ds(i * CH, CH)
            s = own[slot, zp, at].astype(jnp.float32) + part[slot, zp, at].astype(jnp.float32)
            for idx in more:
                s = s + inb[slot, idx, at].astype(jnp.float32)
            own[slot, zp, at] = s.astype(jnp.bfloat16)
            return 0

        lax.fori_loop(0, N // CH, chunk, 0)

    def step_on(slot, k, more):
        wt, layer, _ = place(k)
        base = (k % PER) * N

        def chunk(i, _):
            at = pl.ds(i * CH, CH)
            s = own[slot, z, at].astype(jnp.float32) + part[slot, z, at].astype(jnp.float32)
            for idx in more:
                s = s + inb[slot, idx, at].astype(jnp.float32)
            grad = s.astype(jnp.bfloat16).astype(jnp.float32)
            here = pl.ds(base + i * CH, CH)
            weight = W[wt, layer, me, here].astype(jnp.float32)
            mom = 0.9 * mvb[slot, 0, at] + 0.1 * grad
            var = 0.95 * mvb[slot, 1, at] + 0.05 * grad * grad
            mvb[slot, 0, at] = mom
            mvb[slot, 1, at] = var
            W[wt, layer, me, here] = (weight - 0.02 * (mom * lax.rsqrt(var + 1e-8) + 0.1 * weight)).astype(jnp.bfloat16)
            return 0

        lax.fori_loop(0, N // CH, chunk, 0)

    def block(k, zp, cc):
        wt, layer, at = place(k)
        return W.at[wt, layer, 2 * zp + cc, at]

    def body(t, _):
        t = t - AHEAD

        for zp in range(4):
            k = t - LATE - jnp.where(zp > z, z, 3 - z) * H

            @pl.when(live(k) & (zp != z))
            def _(k=k, zp=zp):
                wait_unit(rs_send.at[k % R, zp])

        @pl.when(live(t))
        def _():
            wait_own(own_sem.at[t % R])
            wait_own(part_recv.at[t % R])
            wait_own(part_send.at[t % R])

        ka = t + AHEAD

        @pl.when(live(ka))
        def _():
            slot = ka % R
            _, layer, at = place(ka)

            def do(i):
                pltpu.make_async_copy(g[i].at[layer, :, c, at], own.at[slot], own_sem.at[slot]).start()
                remote(g[i].at[layer, :, 1 - c, at], part.at[slot], part_send.at[slot], part_recv.at[slot], partner).start()

            of_weight(ka, do)

        ks = t - f_me - LATE

        @pl.when(live(ks))
        def _():
            wait_moment(mv_store.at[ks % R, 0])
            wait_moment(mv_store.at[ks % R, 1])

        km = t - f_me + EARLY

        @pl.when(live(km))
        def _():
            slot = km % R
            _, layer, at = place(km)

            def do(i):
                pltpu.make_async_copy(m[i].at[layer, 0, at], mvb.at[slot, 0], mv_load.at[slot, 0]).start()
                pltpu.make_async_copy(v[i].at[layer, 0, at], mvb.at[slot, 1], mv_load.at[slot, 1]).start()
                pltpu.make_async_copy(w[i].at[layer, me, at], W.at[i, layer, me, at], mv_load.at[slot, 2]).start()

            of_weight(km, do)

        ku, kd = t - z * H, t - (3 - z) * H
        for far in range(3):
            zp = 3 - far

            @pl.when(live(ku) & (zp > z))
            def _(zp=zp):
                slot = ku % R

                @pl.when(z == 0)
                def _():
                    add(slot, zp, ())

                @pl.when(z > 0)
                def _():
                    wait_unit(rs_recv.at[slot, zp])
                    add(slot, zp, (zp,))

                remote(own.at[slot, zp], inb.at[slot, zp], rs_send.at[slot, zp], rs_recv.at[slot, zp], up).start()

            zq = far

            @pl.when(live(kd) & (zq < z))
            def _(zq=zq):
                slot = kd % R

                @pl.when(z == 3)
                def _():
                    add(slot, zq, ())

                @pl.when(z < 3)
                def _():
                    wait_unit(rs_recv.at[slot, zq])
                    add(slot, zq, (zq,))

                idx = jnp.where(zq == z - 1, 4, zq)
                remote(own.at[slot, zq], inb.at[slot, idx], rs_send.at[slot, zq], rs_recv.at[slot, idx], down).start()

        kf = t - f_me

        @pl.when(live(kf))
        def _():
            slot = kf % R
            wait_moment(mv_load.at[slot, 0])
            wait_moment(mv_load.at[slot, 1])
            wait_unit(mv_load.at[slot, 2])

            @pl.when(z > 0)
            def _():
                wait_unit(rs_recv.at[slot, z])

            @pl.when(z < 3)
            def _():
                wait_unit(rs_recv.at[slot, 4])

            @pl.when(z == 0)
            def _():
                step_on(slot, kf, (4,))

            @pl.when(z == 3)
            def _():
                step_on(slot, kf, (3,))

            @pl.when((z > 0) & (z < 3))
            def _():
                step_on(slot, kf, (z, 4))

            mine = block(kf, z, c)

            @pl.when(z < 3)
            def _():
                remote(mine, mine, ag_send.at[slot, z], ag_recv.at[slot, z], up).start()

            @pl.when(z > 0)
            def _():
                remote(mine, mine, ag_send.at[slot, 4], ag_recv.at[slot, z], down).start()

            remote(mine, mine, p_send.at[slot, z], p_recv.at[slot, z], partner).start()
            wt, layer, at = place(kf)

            @pl.when(wt < NV)
            def _():
                for which in range(2):
                    pltpu.make_async_copy(mvb.at[slot, which], MVV.at[which, wt, layer, at], mv_store.at[slot, which]).start()

            @pl.when(wt >= NV)
            def _():
                for which in range(2):
                    pltpu.make_async_copy(mvb.at[slot, which], MV.at[which, wt - NV, layer, at], mv_store.at[slot, which]).start()

        for near in range(3):
            zp = 2 - near
            kb = t - F_OF[zp] - (z - zp) * H

            @pl.when(live(kb) & (zp < z))
            def _(zp=zp, k=kb):
                slot = k % R
                wait_unit(ag_recv.at[slot, zp])
                there = block(k, zp, c)

                @pl.when(z < 3)
                def _():
                    remote(there, there, ag_send.at[slot, zp], ag_recv.at[slot, zp], up).start()

                remote(there, there, p_send.at[slot, zp], p_recv.at[slot, zp], partner).start()

            zq = 1 + near
            kc = t - F_OF[zq] - (zq - z) * H

            @pl.when(live(kc) & (zq > z))
            def _(zq=zq, k=kc):
                slot = k % R
                wait_unit(ag_recv.at[slot, zq])
                there = block(k, zq, c)

                @pl.when(z > 0)
                def _():
                    remote(there, there, ag_send.at[slot, zq], ag_recv.at[slot, zq], down).start()

                remote(there, there, p_send.at[slot, zq], p_recv.at[slot, zq], partner).start()

        for zp in range(4):
            ksent = t - F_OF[zp] - jnp.abs(z - zp) * H

            @pl.when(live(ksent - 1))
            def _(zp=zp, k=ksent - 1):
                wait_unit(p_recv.at[k % R, zp])

            @pl.when(live(ksent - LATE))
            def _(zp=zp, k=ksent - LATE):
                wait_unit(p_send.at[k % R, zp])

                @pl.when((zp < z) & (z < 3))
                def _():
                    wait_unit(ag_send.at[k % R, zp])

                @pl.when((zp > z) & (z > 0))
                def _():
                    wait_unit(ag_send.at[k % R, zp])

                @pl.when((zp == z) & (z < 3))
                def _():
                    wait_unit(ag_send.at[k % R, zp])

                @pl.when((zp == z) & (z > 0))
                def _():
                    wait_unit(ag_send.at[k % R, 4])

        return 0

    lax.fori_loop(0, STEPS + AHEAD, body, 0)


def put_out(*refs):
    W, MVV, MV = refs[0:3]
    whole, rest = refs[3:6], refs[6:12]
    held, load, store, keep = refs[12:16]
    parts = [(which, i, layer) for i in range(NV, 3) for which in range(2) for layer in range(2)]
    for j, (which, i, layer) in enumerate(parts):
        pltpu.make_async_copy(MV.at[which, i - NV, layer], held.at[j], load.at[j]).start()
    copies = [pltpu.make_async_copy(W.at[i], whole[i], keep.at[i]) for i in range(3)]
    for i in range(NV):
        for which in range(2):
            copies.append(pltpu.make_async_copy(MVV.at[which, i], rest[3 * which + i].at[:, 0], keep.at[3 + 2 * i + which]))
    for copy in copies:
        copy.start()
    for j, (which, i, layer) in enumerate(parts):
        pltpu.make_async_copy(MV.at[which, i - NV, layer], held.at[j], load.at[j]).wait()
        copy = pltpu.make_async_copy(held.at[j], rest[3 * which + i].at[layer, 0], store.at[j])
        copy.start()
        copies.append(copy)
    for copy in copies:
        copy.wait()


def solution(mesh):
    def step(*arrays):
        g = [tiled(a[0], 8).reshape(2, 4, 2, UNITS, 16, 128) for a in arrays[:3]]
        w = [tiled(a, 8) for a in arrays[3:6]]
        moments = [tiled(a, 1) for a in arrays[6:]]
        hbm, vmem = pl.BlockSpec(memory_space=pl.ANY), pl.BlockSpec(memory_space=pltpu.VMEM)
        piece = (N, 16, 128)
        dma = pltpu.SemaphoreType.DMA
        new, kept, mv = pl.pallas_call(
            kernel,
            out_shape=[
                pltpu.VMEM((3, 2, 8, UNITS, 16, 128), jnp.bfloat16),
                pltpu.VMEM((2, NV, 2, UNITS, 16, 128), jnp.float32),
                jax.ShapeDtypeStruct((2, 3 - NV, 2, UNITS, 16, 128), jnp.float32),
            ],
            in_specs=[hbm] * 12,
            out_specs=[vmem, vmem, hbm],
            scratch_shapes=[
                pltpu.VMEM((R, 4, *piece), jnp.bfloat16),
                pltpu.VMEM((R, 4, *piece), jnp.bfloat16),
                pltpu.VMEM((R, 5, *piece), jnp.bfloat16),
                pltpu.VMEM((R, 2, *piece), jnp.float32),
                dma((R,)),
                dma((R,)),
                dma((R,)),
                dma((R, 4)),
                dma((R, 5)),
                dma((R, 3)),
                dma((R, 2)),
                dma((R, 5)),
                dma((R, 4)),
                dma((R, 4)),
                dma((R, 4)),
            ],
            compiler_params=pltpu.CompilerParams(collective_id=0, has_side_effects=True, vmem_limit_bytes=int(LIMIT * 2**20)),
            name="sum_step_spread",
        )(*g, *w, *moments)
        parts = 4 * (3 - NV)
        outs = pl.pallas_call(
            put_out,
            out_shape=[jax.ShapeDtypeStruct((2, 8, UNITS, 16, 128), jnp.bfloat16)] * 3 + [jax.ShapeDtypeStruct((2, 1, UNITS, 16, 128), jnp.float32)] * 6,
            in_specs=[vmem, vmem, hbm],
            out_specs=[hbm] * 9,
            scratch_shapes=[pltpu.VMEM((parts, UNITS, 16, 128), jnp.float32), dma((parts,)), dma((parts,)), dma((3 + 2 * NV,))],
            compiler_params=pltpu.CompilerParams(vmem_limit_bytes=int(LIMIT * 2**20)),
            name="put_out",
        )(*(pltpu.with_memory_space_constraint(x, pltpu.VMEM) for x in (new, kept)), pltpu.with_memory_space_constraint(mv, pltpu.HBM))
        whole = [untiled(outs[i], *SHAPES[i]) for i in range(3)]
        rest = [untiled(outs[3 + i], SHAPES[i % 3][0] // 8, SHAPES[i % 3][1]) for i in range(6)]
        return (*whole, *rest)

    all_of, cut = P(None, None, None), P(None, "dp", None)
    return jax.shard_map(
        step,
        mesh=mesh,
        in_specs=(P(("rep", "dp"), None, None, None),) * 3 + (all_of,) * 3 + (cut,) * 6,
        out_specs=(P("rep", None, None),) * 3 + (P("rep", "dp", None),) * 6,
        check_vma=False,
    )
```

```python
import functools

import jax
import jax.numpy as jnp
from jax import lax
from jax.experimental import pallas as pl
from jax.experimental.pallas import tpu as pltpu
from jax.sharding import PartitionSpec as P

MESH = pl.DeviceIdType.MESH
N = 14
UNITS = 224
PER = UNITS // N
K = 6 * PER
H = 1
AHEAD = 1
EARLY = 2
LATE = 3
R = 8
R2 = 6
S = 2
G = 1
ORDER = (0, 1, 2)
CH = 7
NV = 2
LIMIT = 7.75
SHAPES = ((1024, 3584), (1024, 3584), (3584, 1024))
F_OF = (3 * H, 2 * H + S, 2 * H + S, 3 * H)
LAG = (0, S, S, 0)
STEPS = K + max(3 * H + 3 * G, 2 * H + S + 2 * G) + LATE + 1


def tiled(a, blocks):
    layers, rows, columns = a.shape
    a = a.reshape(layers, blocks, rows // blocks // 8, 8, columns // 128, 128).transpose(0, 1, 2, 4, 3, 5)
    return a.reshape(layers, blocks, -1, 16, 128)


def untiled(a, rows, columns):
    layers, blocks = a.shape[:2]
    a = a.reshape(layers, blocks, rows // blocks // 8, columns // 128, 8, 128).transpose(0, 1, 2, 4, 3, 5)
    return a.reshape(layers, rows, columns)


def kernel(*refs):
    g, w, m, v = refs[0:3], refs[3:6], refs[6:9], refs[9:12]
    W, MVV, MV = refs[12:15]
    own, part, inb, mvb = refs[15:19]
    own_sem, part_send, part_recv, rs_send, rs_recv, mv_load, mv_store, ag_send, ag_recv, p_send, p_recv = refs[19:]

    me = lax.axis_index("dp")
    z, c = me // 2, me % 2
    partner = me + 1 - 2 * c
    up, down = jnp.minimum(me + 2, 7), jnp.maximum(me - 2, 0)
    f_me = jnp.where((z == 0) | (z == 3), F_OF[0], F_OF[1])

    def live(k):
        return (k >= 0) & (k < K)

    def place(k):
        return k // (2 * PER), (k // PER) % 2, pl.ds((k % PER) * N, N)

    def of_weight(k, do):
        for i in range(3):
            pl.when(k // (2 * PER) == i)(functools.partial(do, i))

    def remote(src, dst, send, recv, to):
        return pltpu.make_async_remote_copy(src_ref=src, dst_ref=dst, send_sem=send, recv_sem=recv, device_id={"dp": to}, device_id_type=MESH)

    def wait_unit(sem):
        pltpu.make_async_copy(inb.at[0, 0], inb.at[0, 0], sem).wait()

    def wait_own(sem):
        pltpu.make_async_copy(own.at[0], own.at[0], sem).wait()

    def wait_moment(sem):
        pltpu.make_async_copy(mvb.at[0, 0], mvb.at[0, 0], sem).wait()

    def load_own(k):
        slot = k % R
        _, layer, at = place(k)
        of_weight(k, lambda i: pltpu.make_async_copy(g[i].at[layer, :, c, at], own.at[slot], own_sem.at[slot]).start())

    def send_part(k):
        slot = k % R
        _, layer, at = place(k)
        of_weight(k, lambda i: remote(g[i].at[layer, :, 1 - c, at], part.at[slot], part_send.at[slot], part_recv.at[slot], partner).start())

    def load_moments(k):
        slot = k % R2
        _, layer, at = place(k)

        def do(i):
            pltpu.make_async_copy(m[i].at[layer, 0, at], mvb.at[slot, 0], mv_load.at[slot, 0]).start()
            pltpu.make_async_copy(v[i].at[layer, 0, at], mvb.at[slot, 1], mv_load.at[slot, 1]).start()
            pltpu.make_async_copy(w[i].at[layer, me, at], W.at[i, layer, me, at], mv_load.at[slot, 2]).start()

        of_weight(k, do)

    barrier = pltpu.get_barrier_semaphore()
    pl.semaphore_signal(barrier, inc=1, device_id={"dp": partner}, device_id_type=MESH)

    @pl.when(z < 3)
    def _():
        pl.semaphore_signal(barrier, inc=1, device_id={"dp": up}, device_id_type=MESH)

    @pl.when(z > 0)
    def _():
        pl.semaphore_signal(barrier, inc=1, device_id={"dp": down}, device_id_type=MESH)

    for k in range(AHEAD):
        load_own(k)

    pl.semaphore_wait(barrier, jnp.where((z == 0) | (z == 3), 2, 3))

    for k in range(AHEAD):
        send_part(k)

    def add(slot, zp, more):
        def chunk(i, _):
            at = pl.ds(i * CH, CH)
            s = own[slot, zp, at].astype(jnp.float32) + part[slot, zp, at].astype(jnp.float32)
            for idx in more:
                s = s + inb[slot, idx, at].astype(jnp.float32)
            own[slot, zp, at] = s.astype(jnp.bfloat16)
            return 0

        lax.fori_loop(0, N // CH, chunk, 0)

    def step_on(slot, ms, k, more):
        wt, layer, _ = place(k)
        base = (k % PER) * N

        def chunk(i, _):
            at = pl.ds(i * CH, CH)
            s = own[slot, z, at].astype(jnp.float32) + part[slot, z, at].astype(jnp.float32)
            for idx in more:
                s = s + inb[slot, idx, at].astype(jnp.float32)
            grad = s.astype(jnp.bfloat16).astype(jnp.float32)
            here = pl.ds(base + i * CH, CH)
            weight = W[wt, layer, me, here].astype(jnp.float32)
            mom = 0.9 * mvb[ms, 0, at] + 0.1 * grad
            var = 0.95 * mvb[ms, 1, at] + 0.05 * grad * grad
            mvb[ms, 0, at] = mom
            mvb[ms, 1, at] = var
            W[wt, layer, me, here] = (weight - 0.02 * (mom * lax.rsqrt(var + 1e-8) + 0.1 * weight)).astype(jnp.bfloat16)
            return 0

        lax.fori_loop(0, N // CH, chunk, 0)

    def block(k, zp, cc):
        wt, layer, at = place(k)
        return W.at[wt, layer, 2 * zp + cc, at]

    def body(t, _):
        for zp in range(4):
            k = t - LATE - jnp.where(zp > z, z, 3 - z) * H - LAG[zp]

            @pl.when(live(k) & (zp != z))
            def _(k=k, zp=zp):
                wait_unit(rs_send.at[k % R, zp])

        @pl.when(live(t))
        def _():
            wait_own(own_sem.at[t % R])
            wait_own(part_recv.at[t % R])
            wait_own(part_send.at[t % R])

        ka = t + AHEAD

        @pl.when(live(ka))
        def _():
            load_own(ka)
            send_part(ka)

        ks = t - f_me - LATE

        @pl.when(live(ks))
        def _():
            wait_moment(mv_store.at[ks % R2, 0])
            wait_moment(mv_store.at[ks % R2, 1])

        km = t - f_me + EARLY

        @pl.when(live(km))
        def _():
            load_moments(km)

        def sums():
            for far in range(3):
                zp = 3 - far
                ku = t - z * H - LAG[zp]

                @pl.when(live(ku) & (zp > z))
                def _(zp=zp, ku=ku):
                    slot = ku % R

                    @pl.when(z == 0)
                    def _():
                        add(slot, zp, ())

                    @pl.when(z > 0)
                    def _():
                        wait_unit(rs_recv.at[slot, zp])
                        add(slot, zp, (zp,))

                    remote(own.at[slot, zp], inb.at[slot, zp], rs_send.at[slot, zp], rs_recv.at[slot, zp], up).start()

                zq = far
                kd = t - (3 - z) * H - LAG[zq]

                @pl.when(live(kd) & (zq < z))
                def _(zq=zq, kd=kd):
                    slot = kd % R

                    @pl.when(z == 3)
                    def _():
                        add(slot, zq, ())

                    @pl.when(z < 3)
                    def _():
                        wait_unit(rs_recv.at[slot, zq])
                        add(slot, zq, (zq,))

                    idx = jnp.where(zq == z - 1, 4, zq)
                    remote(own.at[slot, zq], inb.at[slot, idx], rs_send.at[slot, zq], rs_recv.at[slot, idx], down).start()

        def take_step():
            kf = t - f_me

            @pl.when(live(kf))
            def _():
                slot, ms = kf % R, kf % R2
                wait_moment(mv_load.at[ms, 0])
                wait_moment(mv_load.at[ms, 1])
                wait_unit(mv_load.at[ms, 2])

                @pl.when(z > 0)
                def _():
                    wait_unit(rs_recv.at[slot, z])

                @pl.when(z < 3)
                def _():
                    wait_unit(rs_recv.at[slot, 4])

                @pl.when(z == 0)
                def _():
                    step_on(slot, ms, kf, (4,))

                @pl.when(z == 3)
                def _():
                    step_on(slot, ms, kf, (3,))

                @pl.when((z > 0) & (z < 3))
                def _():
                    step_on(slot, ms, kf, (z, 4))

                mine = block(kf, z, c)

                @pl.when(z < 3)
                def _():
                    remote(mine, mine, ag_send.at[slot, z], ag_recv.at[slot, z], up).start()

                @pl.when(z > 0)
                def _():
                    remote(mine, mine, ag_send.at[slot, 4], ag_recv.at[slot, z], down).start()

                remote(mine, mine, p_send.at[slot, z], p_recv.at[slot, z], partner).start()
                wt, layer, at = place(kf)

                @pl.when(wt < NV)
                def _():
                    for which in range(2):
                        pltpu.make_async_copy(mvb.at[ms, which], MVV.at[which, wt, layer, at], mv_store.at[ms, which]).start()

                @pl.when(wt >= NV)
                def _():
                    for which in range(2):
                        pltpu.make_async_copy(mvb.at[ms, which], MV.at[which, wt - NV, layer, at], mv_store.at[ms, which]).start()

        def spread():
            for near in range(3):
                zp = 2 - near
                kb = t - F_OF[zp] - (z - zp) * G

                @pl.when(live(kb) & (zp < z))
                def _(zp=zp, k=kb):
                    slot = k % R
                    wait_unit(ag_recv.at[slot, zp])
                    there = block(k, zp, c)

                    @pl.when(z < 3)
                    def _():
                        remote(there, there, ag_send.at[slot, zp], ag_recv.at[slot, zp], up).start()

                    remote(there, there, p_send.at[slot, zp], p_recv.at[slot, zp], partner).start()

                zq = 1 + near
                kc = t - F_OF[zq] - (zq - z) * G

                @pl.when(live(kc) & (zq > z))
                def _(zq=zq, k=kc):
                    slot = k % R
                    wait_unit(ag_recv.at[slot, zq])
                    there = block(k, zq, c)

                    @pl.when(z > 0)
                    def _():
                        remote(there, there, ag_send.at[slot, zq], ag_recv.at[slot, zq], down).start()

                    remote(there, there, p_send.at[slot, zq], p_recv.at[slot, zq], partner).start()

        for i in ORDER:
            (sums, take_step, spread)[i]()

        for zp in range(4):
            ksent = t - F_OF[zp] - jnp.abs(z - zp) * G

            @pl.when(live(ksent - 1))
            def _(zp=zp, k=ksent - 1):
                wait_unit(p_recv.at[k % R, zp])

            @pl.when(live(ksent - LATE))
            def _(zp=zp, k=ksent - LATE):
                wait_unit(p_send.at[k % R, zp])

                @pl.when((zp < z) & (z < 3))
                def _():
                    wait_unit(ag_send.at[k % R, zp])

                @pl.when((zp > z) & (z > 0))
                def _():
                    wait_unit(ag_send.at[k % R, zp])

                @pl.when((zp == z) & (z < 3))
                def _():
                    wait_unit(ag_send.at[k % R, zp])

                @pl.when((zp == z) & (z > 0))
                def _():
                    wait_unit(ag_send.at[k % R, 4])

        return 0

    lax.fori_loop(0, STEPS, body, 0)


def put_out(*refs):
    W, MVV, MV = refs[0:3]
    whole, rest = refs[3:6], refs[6:12]
    held, load, store, keep = refs[12:16]
    parts = [(which, i, layer) for i in range(NV, 3) for which in range(2) for layer in range(2)]
    for j, (which, i, layer) in enumerate(parts):
        pltpu.make_async_copy(MV.at[which, i - NV, layer], held.at[j], load.at[j]).start()
    copies = [pltpu.make_async_copy(W.at[i, l], whole[i].at[l], keep.at[7 + 2 * i + l]) for i in range(3) for l in range(2)]
    for i in range(NV):
        for which in range(2):
            copies.append(pltpu.make_async_copy(MVV.at[which, i], rest[3 * which + i].at[:, 0], keep.at[3 + 2 * i + which]))
    for copy in copies:
        copy.start()
    for j, (which, i, layer) in enumerate(parts):
        pltpu.make_async_copy(MV.at[which, i - NV, layer], held.at[j], load.at[j]).wait()
        copy = pltpu.make_async_copy(held.at[j], rest[3 * which + i].at[layer, 0], store.at[j])
        copy.start()
        copies.append(copy)
    for copy in copies:
        copy.wait()


def solution(mesh):
    def step(*arrays):
        g = [tiled(a[0], 8).reshape(2, 4, 2, UNITS, 16, 128) for a in arrays[:3]]
        w = [tiled(a, 8) for a in arrays[3:6]]
        moments = [tiled(a, 1) for a in arrays[6:]]
        hbm, vmem = pl.BlockSpec(memory_space=pl.ANY), pl.BlockSpec(memory_space=pltpu.VMEM)
        piece = (N, 16, 128)
        dma = pltpu.SemaphoreType.DMA
        new, kept, mv = pl.pallas_call(
            kernel,
            out_shape=[
                pltpu.VMEM((3, 2, 8, UNITS, 16, 128), jnp.bfloat16),
                pltpu.VMEM((2, NV, 2, UNITS, 16, 128), jnp.float32),
                jax.ShapeDtypeStruct((2, 3 - NV, 2, UNITS, 16, 128), jnp.float32),
            ],
            in_specs=[hbm] * 12,
            out_specs=[vmem, vmem, hbm],
            scratch_shapes=[
                pltpu.VMEM((R, 4, *piece), jnp.bfloat16),
                pltpu.VMEM((R, 4, *piece), jnp.bfloat16),
                pltpu.VMEM((R, 5, *piece), jnp.bfloat16),
                pltpu.VMEM((R2, 2, *piece), jnp.float32),
                dma((R,)),
                dma((R,)),
                dma((R,)),
                dma((R, 4)),
                dma((R, 5)),
                dma((R2, 3)),
                dma((R2, 2)),
                dma((R, 5)),
                dma((R, 4)),
                dma((R, 4)),
                dma((R, 4)),
            ],
            compiler_params=pltpu.CompilerParams(collective_id=0, has_side_effects=True, vmem_limit_bytes=int(LIMIT * 2**20)),
            name="sum_step_spread",
        )(*g, *w, *moments)
        parts = 4 * (3 - NV)
        outs = pl.pallas_call(
            put_out,
            out_shape=[jax.ShapeDtypeStruct((2, 8, UNITS, 16, 128), jnp.bfloat16)] * 3 + [jax.ShapeDtypeStruct((2, 1, UNITS, 16, 128), jnp.float32)] * 6,
            in_specs=[vmem, vmem, hbm],
            out_specs=[hbm] * 9,
            scratch_shapes=[pltpu.VMEM((parts, UNITS, 16, 128), jnp.float32), dma((parts,)), dma((parts,)), dma((13,))],
            compiler_params=pltpu.CompilerParams(vmem_limit_bytes=int(LIMIT * 2**20)),
            name="put_out",
        )(*(pltpu.with_memory_space_constraint(x, pltpu.VMEM) for x in (new, kept)), pltpu.with_memory_space_constraint(mv, pltpu.HBM))
        whole = [untiled(outs[i], *SHAPES[i]) for i in range(3)]
        rest = [untiled(outs[3 + i], SHAPES[i % 3][0] // 8, SHAPES[i % 3][1]) for i in range(6)]
        return (*whole, *rest)

    all_of, cut = P(None, None, None), P(None, "dp", None)
    return jax.shard_map(
        step,
        mesh=mesh,
        in_specs=(P(("rep", "dp"), None, None, None),) * 3 + (all_of,) * 3 + (cut,) * 6,
        out_specs=(P("rep", None, None),) * 3 + (P("rep", "dp", None),) * 6,
        check_vma=False,
    )
```

```python
import functools

import jax
import jax.numpy as jnp
from jax import lax
from jax.experimental import pallas as pl
from jax.experimental.pallas import tpu as pltpu
from jax.sharding import PartitionSpec as P

MESH = pl.DeviceIdType.MESH
N = 14
UNITS = 224
PER = UNITS // N
K = 6 * PER
H = 1
AHEAD = 1
FIRST = 4
EARLY = 2
LATE = 3
R = 8
R2 = 6
S = 2
G = 1
ORDER = (0, 1, 2)
CH = 14
NV = 2
LIMIT = 7.75
SHAPES = ((1024, 3584), (1024, 3584), (3584, 1024))
F_OF = (3 * H, 2 * H + S, 2 * H + S, 3 * H)
LAG = (0, S, S, 0)
STEPS = K + max(3 * H + 3 * G, 2 * H + S + 2 * G) + LATE + 1


def tiled(a, blocks):
    layers, rows, columns = a.shape
    a = a.reshape(layers, blocks, rows // blocks // 8, 8, columns // 128, 128).transpose(0, 1, 2, 4, 3, 5)
    return a.reshape(layers, blocks, -1, 16, 128)


def untiled(a, rows, columns):
    layers, blocks = a.shape[:2]
    a = a.reshape(layers, blocks, rows // blocks // 8, columns // 128, 8, 128).transpose(0, 1, 2, 4, 3, 5)
    return a.reshape(layers, rows, columns)


def kernel(*refs):
    g, w, m, v = refs[0:3], refs[3:6], refs[6:9], refs[9:12]
    W, MVV, MV = refs[12:15]
    own, part, inb, mvb = refs[15:19]
    own_sem, part_send, part_recv, rs_send, rs_recv, mv_load, mv_store, ag_send, ag_recv, p_send, p_recv = refs[19:]

    me = lax.axis_index("dp")
    z, c = me // 2, me % 2
    partner = me + 1 - 2 * c
    up, down = jnp.minimum(me + 2, 7), jnp.maximum(me - 2, 0)
    f_me = jnp.where((z == 0) | (z == 3), F_OF[0], F_OF[1])

    def live(k):
        return (k >= 0) & (k < K)

    def place(k):
        return k // (2 * PER), (k // PER) % 2, pl.ds((k % PER) * N, N)

    def of_weight(k, do):
        for i in range(3):
            pl.when(k // (2 * PER) == i)(functools.partial(do, i))

    def remote(src, dst, send, recv, to):
        return pltpu.make_async_remote_copy(src_ref=src, dst_ref=dst, send_sem=send, recv_sem=recv, device_id={"dp": to}, device_id_type=MESH)

    def wait_unit(sem):
        pltpu.make_async_copy(inb.at[0, 0], inb.at[0, 0], sem).wait()

    def wait_own(sem):
        pltpu.make_async_copy(own.at[0], own.at[0], sem).wait()

    def wait_moment(sem):
        pltpu.make_async_copy(mvb.at[0, 0], mvb.at[0, 0], sem).wait()

    def load_own(k):
        slot = k % R
        _, layer, at = place(k)
        of_weight(k, lambda i: pltpu.make_async_copy(g[i].at[layer, :, c, at], own.at[slot], own_sem.at[slot]).start())

    def send_part(k):
        slot = k % R
        _, layer, at = place(k)
        of_weight(k, lambda i: remote(g[i].at[layer, :, 1 - c, at], part.at[slot], part_send.at[slot], part_recv.at[slot], partner).start())

    def load_moments(k):
        slot = k % R2
        _, layer, at = place(k)

        def do(i):
            pltpu.make_async_copy(m[i].at[layer, 0, at], mvb.at[slot, 0], mv_load.at[slot, 0]).start()
            pltpu.make_async_copy(v[i].at[layer, 0, at], mvb.at[slot, 1], mv_load.at[slot, 1]).start()
            pltpu.make_async_copy(w[i].at[layer, me, at], W.at[i, layer, me, at], mv_load.at[slot, 2]).start()

        of_weight(k, do)

    barrier = pltpu.get_barrier_semaphore()
    pl.semaphore_signal(barrier, inc=1, device_id={"dp": partner}, device_id_type=MESH)

    @pl.when(z < 3)
    def _():
        pl.semaphore_signal(barrier, inc=1, device_id={"dp": up}, device_id_type=MESH)

    @pl.when(z > 0)
    def _():
        pl.semaphore_signal(barrier, inc=1, device_id={"dp": down}, device_id_type=MESH)

    for k in range(FIRST):
        load_own(k)

    pl.semaphore_wait(barrier, jnp.where((z == 0) | (z == 3), 2, 3))

    for k in range(FIRST):
        send_part(k)

    def add(slot, zp, more):
        def chunk(i, _):
            at = pl.ds(i * CH, CH)
            s = own[slot, zp, at].astype(jnp.float32) + part[slot, zp, at].astype(jnp.float32)
            for idx in more:
                s = s + inb[slot, idx, at].astype(jnp.float32)
            own[slot, zp, at] = s.astype(jnp.bfloat16)
            return 0

        lax.fori_loop(0, N // CH, chunk, 0)

    def step_on(slot, ms, k, more):
        wt, layer, _ = place(k)
        base = (k % PER) * N

        def chunk(i, _):
            at = pl.ds(i * CH, CH)
            s = own[slot, z, at].astype(jnp.float32) + part[slot, z, at].astype(jnp.float32)
            for idx in more:
                s = s + inb[slot, idx, at].astype(jnp.float32)
            grad = s.astype(jnp.bfloat16).astype(jnp.float32)
            here = pl.ds(base + i * CH, CH)
            weight = W[wt, layer, me, here].astype(jnp.float32)
            mom = 0.9 * mvb[ms, 0, at] + 0.1 * grad
            var = 0.95 * mvb[ms, 1, at] + 0.05 * grad * grad
            mvb[ms, 0, at] = mom
            mvb[ms, 1, at] = var
            W[wt, layer, me, here] = (weight - 0.02 * (mom * lax.rsqrt(var + 1e-8) + 0.1 * weight)).astype(jnp.bfloat16)
            return 0

        lax.fori_loop(0, N // CH, chunk, 0)

    def block(k, zp, cc):
        wt, layer, at = place(k)
        return W.at[wt, layer, 2 * zp + cc, at]

    def body(t, _):
        for zp in range(4):
            k = t - LATE - jnp.where(zp > z, z, 3 - z) * H - LAG[zp]

            @pl.when(live(k) & (zp != z))
            def _(k=k, zp=zp):
                wait_unit(rs_send.at[k % R, zp])

        @pl.when(live(t))
        def _():
            wait_own(own_sem.at[t % R])
            wait_own(part_recv.at[t % R])
            wait_own(part_send.at[t % R])

        ka = t + AHEAD

        @pl.when(live(ka) & (ka >= FIRST))
        def _():
            load_own(ka)
            send_part(ka)

        ks = t - f_me - LATE

        @pl.when(live(ks))
        def _():
            wait_moment(mv_store.at[ks % R2, 0])
            wait_moment(mv_store.at[ks % R2, 1])

        km = t - f_me + EARLY

        @pl.when(live(km))
        def _():
            load_moments(km)

        def sums():
            for far in range(3):
                zp = 3 - far
                ku = t - z * H - LAG[zp]

                @pl.when(live(ku) & (zp > z))
                def _(zp=zp, ku=ku):
                    slot = ku % R

                    @pl.when(z == 0)
                    def _():
                        add(slot, zp, ())

                    @pl.when(z > 0)
                    def _():
                        wait_unit(rs_recv.at[slot, zp])
                        add(slot, zp, (zp,))

                    remote(own.at[slot, zp], inb.at[slot, zp], rs_send.at[slot, zp], rs_recv.at[slot, zp], up).start()

                zq = far
                kd = t - (3 - z) * H - LAG[zq]

                @pl.when(live(kd) & (zq < z))
                def _(zq=zq, kd=kd):
                    slot = kd % R

                    @pl.when(z == 3)
                    def _():
                        add(slot, zq, ())

                    @pl.when(z < 3)
                    def _():
                        wait_unit(rs_recv.at[slot, zq])
                        add(slot, zq, (zq,))

                    idx = jnp.where(zq == z - 1, 4, zq)
                    remote(own.at[slot, zq], inb.at[slot, idx], rs_send.at[slot, zq], rs_recv.at[slot, idx], down).start()

        def take_step():
            kf = t - f_me

            @pl.when(live(kf))
            def _():
                slot, ms = kf % R, kf % R2
                wait_moment(mv_load.at[ms, 0])
                wait_moment(mv_load.at[ms, 1])
                wait_unit(mv_load.at[ms, 2])

                @pl.when(z > 0)
                def _():
                    wait_unit(rs_recv.at[slot, z])

                @pl.when(z < 3)
                def _():
                    wait_unit(rs_recv.at[slot, 4])

                @pl.when(z == 0)
                def _():
                    step_on(slot, ms, kf, (4,))

                @pl.when(z == 3)
                def _():
                    step_on(slot, ms, kf, (3,))

                @pl.when((z > 0) & (z < 3))
                def _():
                    step_on(slot, ms, kf, (z, 4))

                mine = block(kf, z, c)

                @pl.when(z < 3)
                def _():
                    remote(mine, mine, ag_send.at[slot, z], ag_recv.at[slot, z], up).start()

                @pl.when(z > 0)
                def _():
                    remote(mine, mine, ag_send.at[slot, 4], ag_recv.at[slot, z], down).start()

                remote(mine, mine, p_send.at[slot, z], p_recv.at[slot, z], partner).start()
                wt, layer, at = place(kf)

                @pl.when(wt < NV)
                def _():
                    for which in range(2):
                        pltpu.make_async_copy(mvb.at[ms, which], MVV.at[which, wt, layer, at], mv_store.at[ms, which]).start()

                @pl.when(wt >= NV)
                def _():
                    for which in range(2):
                        pltpu.make_async_copy(mvb.at[ms, which], MV.at[which, wt - NV, layer, at], mv_store.at[ms, which]).start()

        def spread():
            for near in range(3):
                zp = 2 - near
                kb = t - F_OF[zp] - (z - zp) * G

                @pl.when(live(kb) & (zp < z))
                def _(zp=zp, k=kb):
                    slot = k % R
                    wait_unit(ag_recv.at[slot, zp])
                    there = block(k, zp, c)

                    @pl.when(z < 3)
                    def _():
                        remote(there, there, ag_send.at[slot, zp], ag_recv.at[slot, zp], up).start()

                    remote(there, there, p_send.at[slot, zp], p_recv.at[slot, zp], partner).start()

                zq = 1 + near
                kc = t - F_OF[zq] - (zq - z) * G

                @pl.when(live(kc) & (zq > z))
                def _(zq=zq, k=kc):
                    slot = k % R
                    wait_unit(ag_recv.at[slot, zq])
                    there = block(k, zq, c)

                    @pl.when(z > 0)
                    def _():
                        remote(there, there, ag_send.at[slot, zq], ag_recv.at[slot, zq], down).start()

                    remote(there, there, p_send.at[slot, zq], p_recv.at[slot, zq], partner).start()

        for i in ORDER:
            (sums, take_step, spread)[i]()

        for zp in range(4):
            ksent = t - F_OF[zp] - jnp.abs(z - zp) * G

            @pl.when(live(ksent - 1))
            def _(zp=zp, k=ksent - 1):
                wait_unit(p_recv.at[k % R, zp])

            @pl.when(live(ksent - LATE))
            def _(zp=zp, k=ksent - LATE):
                wait_unit(p_send.at[k % R, zp])

                @pl.when((zp < z) & (z < 3))
                def _():
                    wait_unit(ag_send.at[k % R, zp])

                @pl.when((zp > z) & (z > 0))
                def _():
                    wait_unit(ag_send.at[k % R, zp])

                @pl.when((zp == z) & (z < 3))
                def _():
                    wait_unit(ag_send.at[k % R, zp])

                @pl.when((zp == z) & (z > 0))
                def _():
                    wait_unit(ag_send.at[k % R, 4])

        return 0

    lax.fori_loop(0, STEPS, body, 0)


def put_out(*refs):
    W, MVV, MV = refs[0:3]
    whole, rest = refs[3:6], refs[6:12]
    held, load, store, keep = refs[12:16]
    parts = [(which, i, layer) for i in range(NV, 3) for which in range(2) for layer in range(2)]
    for j, (which, i, layer) in enumerate(parts):
        pltpu.make_async_copy(MV.at[which, i - NV, layer], held.at[j], load.at[j]).start()
    copies = [pltpu.make_async_copy(W.at[i, l], whole[i].at[l], keep.at[7 + 2 * i + l]) for i in range(3) for l in range(2)]
    for i in range(NV):
        for which in range(2):
            copies.append(pltpu.make_async_copy(MVV.at[which, i], rest[3 * which + i].at[:, 0], keep.at[3 + 2 * i + which]))
    for copy in copies:
        copy.start()
    for j, (which, i, layer) in enumerate(parts):
        pltpu.make_async_copy(MV.at[which, i - NV, layer], held.at[j], load.at[j]).wait()
        copy = pltpu.make_async_copy(held.at[j], rest[3 * which + i].at[layer, 0], store.at[j])
        copy.start()
        copies.append(copy)
    for copy in copies:
        copy.wait()


def solution(mesh):
    def step(*arrays):
        g = [tiled(a[0], 8).reshape(2, 4, 2, UNITS, 16, 128) for a in arrays[:3]]
        w = [tiled(a, 8) for a in arrays[3:6]]
        moments = [tiled(a, 1) for a in arrays[6:]]
        hbm, vmem = pl.BlockSpec(memory_space=pl.ANY), pl.BlockSpec(memory_space=pltpu.VMEM)
        piece = (N, 16, 128)
        dma = pltpu.SemaphoreType.DMA
        new, kept, mv = pl.pallas_call(
            kernel,
            out_shape=[
                pltpu.VMEM((3, 2, 8, UNITS, 16, 128), jnp.bfloat16),
                pltpu.VMEM((2, NV, 2, UNITS, 16, 128), jnp.float32),
                jax.ShapeDtypeStruct((2, 3 - NV, 2, UNITS, 16, 128), jnp.float32),
            ],
            in_specs=[hbm] * 12,
            out_specs=[vmem, vmem, hbm],
            scratch_shapes=[
                pltpu.VMEM((R, 4, *piece), jnp.bfloat16),
                pltpu.VMEM((R, 4, *piece), jnp.bfloat16),
                pltpu.VMEM((R, 5, *piece), jnp.bfloat16),
                pltpu.VMEM((R2, 2, *piece), jnp.float32),
                dma((R,)),
                dma((R,)),
                dma((R,)),
                dma((R, 4)),
                dma((R, 5)),
                dma((R2, 3)),
                dma((R2, 2)),
                dma((R, 5)),
                dma((R, 4)),
                dma((R, 4)),
                dma((R, 4)),
            ],
            compiler_params=pltpu.CompilerParams(collective_id=0, has_side_effects=True, vmem_limit_bytes=int(LIMIT * 2**20)),
            name="sum_step_spread",
        )(*g, *w, *moments)
        parts = 4 * (3 - NV)
        outs = pl.pallas_call(
            put_out,
            out_shape=[jax.ShapeDtypeStruct((2, 8, UNITS, 16, 128), jnp.bfloat16)] * 3 + [jax.ShapeDtypeStruct((2, 1, UNITS, 16, 128), jnp.float32)] * 6,
            in_specs=[vmem, vmem, hbm],
            out_specs=[hbm] * 9,
            scratch_shapes=[pltpu.VMEM((parts, UNITS, 16, 128), jnp.float32), dma((parts,)), dma((parts,)), dma((13,))],
            compiler_params=pltpu.CompilerParams(vmem_limit_bytes=int(LIMIT * 2**20)),
            name="put_out",
        )(*(pltpu.with_memory_space_constraint(x, pltpu.VMEM) for x in (new, kept)), pltpu.with_memory_space_constraint(mv, pltpu.HBM))
        whole = [untiled(outs[i], *SHAPES[i]) for i in range(3)]
        rest = [untiled(outs[3 + i], SHAPES[i % 3][0] // 8, SHAPES[i % 3][1]) for i in range(6)]
        return (*whole, *rest)

    all_of, cut = P(None, None, None), P(None, "dp", None)
    return jax.shard_map(
        step,
        mesh=mesh,
        in_specs=(P(("rep", "dp"), None, None, None),) * 3 + (all_of,) * 3 + (cut,) * 6,
        out_specs=(P("rep", None, None),) * 3 + (P("rep", "dp", None),) * 6,
        check_vma=False,
    )
```
